32 devices in a mesh: seq: 8 (over z, y), tp: 4 (over x, core).
Axes of the slice: x: 2, y: 2, z: 4, core: 2. Of those that a mesh axis runs over, the one named last changes fastest.
Arguments:
- tokens: bfloat16 [6144, 4096], P('seq'), may hold values from -6 to 6
- query_weight: bfloat16 [4096, 2048], P('seq', 'tp'), may hold values from -0.09375 to 0.09375
- key_weight: bfloat16 [4096, 2048], P('seq', 'tp'), may hold values from -0.09375 to 0.09375
- value_weight: bfloat16 [4096, 2048], P('seq', 'tp'), may hold values from -0.09375 to 0.09375
- gate_weight: bfloat16 [4096, 16], P('seq', 'tp'), may hold values from -0.09375 to 0.09375
- decay_rate: float32 [16], P('tp'), may hold values from 3.2552085e-05 to 0.04
- norm_gain: float32 [2048], P('tp'), may hold values from 0.5 to 1.5
- out_weight: bfloat16 [2048, 4096], P(None, 'tp'), may hold values from -0.125 to 0.125
Outputs:
- mixed: bfloat16 [6144, 4096], P('seq', 'tp')
The draws below stay inside these ranges and needn't reach their ends.
All inputs are finite; a program needn't handle non-finite values.
Results may differ from the reference program's by a relative error of at most 0.006.
The reference program's roundings to bfloat16 on the way count: a program that leaves them out, or rounds other values in their place, can miss the bound.
Values may be sent and summed in bfloat16 or wider, within the bound.
No kernel may reach another device: no remote copies, remote signals or barrier semaphores. Data moves between devices by JAX's collectives and lax.ppermute only.
A program may use at most 128 MiB of HBM per device.

```python
import math
import jax
import jax.numpy as jnp
from jax import lax

D = 4096
H = 16
K = 128
TOK_DEV = 768
TOKENS = 6144


def level_of(own_key, shape, shards, smallest, high):
    def one(dim, blocks):
        steps = jax.random.uniform(jax.random.fold_in(jax.random.fold_in(own_key, 6), dim), (blocks,), jnp.float32, smallest / len(shards), high / len(shards))
        return jnp.repeat(jnp.exp(steps), shape[dim] // blocks).reshape((-1,) + (1,) * (len(shape) - dim - 1))

    level = one(*shards[0])
    for cut in shards[1:]:
        level = level * one(*cut)
    return level


def centred(own_key, dims, spread, reach, pieces=(), kind=jnp.bfloat16):
    loudness = level_of(own_key, dims, pieces, -0.22, 0.18) if pieces else 1.0
    values = jax.random.normal(own_key, dims, jnp.float32) * spread * loudness
    return jnp.minimum(jnp.maximum(values, -reach), reach).astype(kind)


def setup_inputs(seed: int = 0) -> dict:
    key_of = jax.random.split(jax.random.key(seed), 9)
    return {
        "tokens": centred(key_of[0], (TOKENS, D), 1.0, 6.0, ((0, 8),)),
        "query_weight": centred(key_of[1], (D, H * K), D ** -0.5, 0.09375, ((0, 8), (1, 4))),
        "key_weight": centred(key_of[2], (D, H * K), D ** -0.5, 0.09375, ((0, 8), (1, 4))),
        "value_weight": centred(key_of[3], (D, H * K), D ** -0.5, 0.09375, ((0, 8), (1, 4))),
        "gate_weight": centred(key_of[4], (D, H), D ** -0.5, 0.09375, ((0, 8), (1, 4))),
        "decay_rate": jnp.clip(jnp.exp(math.log(0.04) - 7.1137933 * jax.random.uniform(key_of[5], (H,), jnp.float32) ** level_of(key_of[5], (H,), ((0, 4),), -0.2, 0.2)), 3.255208503105678e-05, 0.04),
        "norm_gain": jnp.clip(1.0 + 0.1 * jax.random.normal(key_of[6], (H * K,), jnp.float32), 0.5, 1.5),
        "out_weight": centred(key_of[7], (H * K, D), (H * K) ** -0.5, 0.125, ((1, 4),)),
    }


def reference(tokens, query_weight, key_weight, value_weight, gate_weight, decay_rate, norm_gain, out_weight):
    query_proj = jnp.dot(tokens, query_weight, preferred_element_type=jnp.float32).astype(jnp.bfloat16)
    key_proj = jnp.dot(tokens, key_weight, preferred_element_type=jnp.float32).astype(jnp.bfloat16)
    value_proj = jnp.dot(tokens, value_weight, preferred_element_type=jnp.float32).astype(jnp.bfloat16)
    gate_logit = jnp.dot(tokens, gate_weight, preferred_element_type=jnp.float32)
    log_decay = -decay_rate[None, :] * jax.nn.softplus(gate_logit)
    block_count = TOKENS // TOK_DEV
    query_blocks = query_proj.reshape(block_count, TOK_DEV, H, K)
    key_blocks = key_proj.reshape(block_count, TOK_DEV, H, K)
    value_blocks = value_proj.reshape(block_count, TOK_DEV, H, K)
    decay_blocks = log_decay.reshape(block_count, TOK_DEV, H)
    causal = jnp.tril(jnp.ones((TOK_DEV, TOK_DEV), dtype=bool))[None, :, :]

    def block_step(prev_state, items):
        query_blk, key_blk, value_blk, decay_blk = items
        within = jnp.cumsum(decay_blk, axis=0)
        block_total = within[-1]
        query_wide = query_blk.astype(jnp.float32)
        key_wide = key_blk.astype(jnp.float32)
        value_full_width = value_blk.astype(jnp.float32)
        query_scaled = (jnp.exp(within)[:, :, None] * query_wide).astype(jnp.bfloat16)
        state_bfloat = prev_state.astype(jnp.bfloat16)
        carried_state = jnp.einsum('fys,ysu->fyu', query_scaled.astype(jnp.float32), state_bfloat.astype(jnp.float32))
        scores = jnp.einsum('thk,shk->hts', query_wide, key_wide)
        decay_gap = within.T[:, :, None] - within.T[:, None, :]
        attn = jnp.where(causal, scores * jnp.exp(jnp.where(causal, decay_gap, 0.0)), 0.0).astype(jnp.bfloat16)
        local_part = jnp.einsum('hts,shv->thv', attn.astype(jnp.float32), value_full_width)
        key_scaled = (jnp.exp(block_total[None, :] - within)[:, :, None] * key_wide).astype(jnp.bfloat16)
        shard_local_state = jnp.einsum('gfw,gfz->fwz', key_scaled.astype(jnp.float32), value_full_width)
        next_state = jnp.exp(block_total)[:, None, None] * prev_state + shard_local_state
        return (next_state, carried_state + local_part)
    start_state = jnp.zeros((H, K, K), jnp.float32)
    _, head_out = lax.scan(block_step, start_state, (query_blocks, key_blocks, value_blocks, decay_blocks))
    mean_square = lax.optimization_barrier(jnp.mean(head_out * head_out, axis=-1, keepdims=True))
    normed = (head_out * lax.rsqrt(mean_square + 1e-05)).reshape(TOKENS, H * K) * norm_gain[None, :]
    normed = normed.astype(jnp.bfloat16)
    return jnp.dot(normed, out_weight, preferred_element_type=jnp.float32).astype(jnp.bfloat16)
```

```python
import functools
import math

import jax
import jax.numpy as jnp
from jax import lax
from jax.experimental import pallas as pl
from jax.experimental.pallas import tpu as pltpu
from jax.sharding import PartitionSpec as P

BF = jnp.bfloat16
F32 = jnp.float32


def project_kernel(where, tok_ref, *refs, planes):
    block_refs, out_ref = refs[:-1], refs[-1]
    plane, half = where[0], where[1]
    rows = block_refs[0].shape[0]
    merged = len(block_refs) == planes
    acc = None
    for i, block_ref in enumerate(block_refs):
        if merged:
            block = lax.rem(plane + i, planes)
        else:
            block = lax.rem(plane + i // 2, planes) * 2 + (half if i % 2 == 0 else 1 - half)
        start = pl.multiple_of(block * rows, rows)
        part = jnp.dot(
            tok_ref[:, pl.ds(start, rows)], block_ref[...], preferred_element_type=F32
        )
        acc = part if acc is None else acc + part
    out_ref[...] = acc.astype(out_ref.dtype)


def project(where, tok, blocks, planes):
    tok_rows, width = tok.shape
    cols = blocks[0].shape[1]
    tile = math.gcd(tok_rows, 384)
    if blocks[0].shape[0] % 128:
        first = where[1] == 0
        blocks = [
            jnp.concatenate([jnp.where(first, a, b), jnp.where(first, b, a)], axis=0)
            for a, b in zip(blocks[0::2], blocks[1::2])
        ]
    return pl.pallas_call(
        functools.partial(project_kernel, planes=planes),
        out_shape=jax.ShapeDtypeStruct((tok_rows, cols), BF),
        grid_spec=pltpu.PrefetchScalarGridSpec(
            num_scalar_prefetch=1,
            grid=(tok_rows // tile,),
            in_specs=[pl.BlockSpec((tile, width), lambda i, w: (i, 0))]
            + [pl.BlockSpec(b.shape, lambda i, w: (0, 0)) for b in blocks],
            out_specs=pl.BlockSpec((tile, cols), lambda i, w: (i, 0)),
        ),
        compiler_params=pltpu.CompilerParams(vmem_limit_bytes=40 * 2**20),
        cost_estimate=pl.CostEstimate(
            flops=2 * tok_rows * width * cols,
            bytes_accessed=2 * (tok_rows * width + width * cols + tok_rows * cols),
            transcendentals=0,
        ),
        name="project",
    )(where, tok, *blocks)


def mix_kernel(q_ref, k_ref, v_ref, wide_ref, row_ref, state_ref, gain_ref, out_ref, *, tile):
    tok_rows = q_ref.shape[0]
    for i in range(tok_rows // tile):
        lo, hi = i * tile, (i + 1) * tile
        query = q_ref[lo:hi, :]
        wide = wide_ref[lo:hi, :]
        scores = lax.dot_general(
            query, k_ref[0:hi, :], (((1,), (1,)), ((), ())), preferred_element_type=F32
        )
        gap = wide[:, 0:1] - row_ref[0:1, 0:hi]
        row_index = lo + lax.broadcasted_iota(jnp.int32, (tile, hi), 0)
        col_index = lax.broadcasted_iota(jnp.int32, (tile, hi), 1)
        causal = col_index <= row_index
        attn = jnp.where(causal, scores * jnp.exp(jnp.where(causal, gap, 0.0)), 0.0).astype(BF)
        local = jnp.dot(attn, v_ref[0:hi, :], preferred_element_type=F32)
        scaled = (jnp.exp(wide) * query.astype(F32)).astype(BF)
        carried = jnp.dot(scaled, state_ref[...], preferred_element_type=F32)
        head_out = carried + local
        mean_square = jnp.mean(head_out * head_out, axis=-1, keepdims=True)
        normed = head_out * lax.rsqrt(mean_square + 1e-05) * gain_ref[...]
        out_ref[lo:hi, :] = normed.astype(BF)


def mix(query, key, value, wide, row, state, gain):
    tok_rows, head_size = query.shape
    return pl.pallas_call(
        functools.partial(mix_kernel, tile=math.gcd(tok_rows, 256)),
        out_shape=jax.ShapeDtypeStruct((tok_rows, head_size), BF),
        compiler_params=pltpu.CompilerParams(vmem_limit_bytes=32 * 2**20),
        cost_estimate=pl.CostEstimate(
            flops=4 * tok_rows * tok_rows * head_size,
            bytes_accessed=tok_rows * head_size * 12,
            transcendentals=tok_rows * tok_rows,
        ),
        name="mix",
    )(query, key, value, wide, row, state, gain)


def solution(mesh):
    n_seq, n_tp = mesh.shape["seq"], mesh.shape["tp"]
    planes = n_seq // 2

    def from_plane(step):
        return [(2 * ((z + step) % planes) + y, 2 * z + y) for z in range(planes) for y in (0, 1)]

    half_swap = [(s, s ^ 1) for s in range(n_seq)]
    pair_swap = [(s, s ^ 2) for s in range(n_seq)]
    quad_up = [(s, s + 4) for s in range(n_seq - 4)]

    def over_tp(own):
        got = {0: own}
        bit = n_tp // 2
        while bit:
            swap = [(t, t ^ bit) for t in range(n_tp)]
            got.update({i ^ bit: lax.ppermute(v, "tp", swap) for i, v in list(got.items())})
            bit //= 2
        return [got[i] for i in range(n_tp)]

    def on_device(
        tokens, query_weight, key_weight, value_weight, gate_weight, decay_rate, norm_gain, out_weight
    ):
        tok_rows, width = tokens.shape
        heads = decay_rate.shape[0]
        hp = heads // 2
        size = query_weight.shape[1] // heads
        rank = lax.axis_index("seq")
        tp = lax.axis_index("tp")
        half = rank % 2
        plane = rank // 2
        par = plane % 2
        where = jnp.stack([plane, half]).astype(jnp.int32)

        gate = gate_weight.T
        gate_z = jnp.stack([gate] + [lax.ppermute(gate, "seq", from_plane(k)) for k in range(1, planes)])
        gate_zy = lax.ppermute(gate_z, "seq", half_swap)
        low = jnp.where(half == 0, gate_z, gate_zy)
        high = jnp.where(half == 0, gate_zy, gate_z)
        gate_all = jnp.concatenate([low, high], axis=2)
        gate_all = lax.dynamic_slice_in_dim(
            jnp.concatenate([gate_all, gate_all], axis=0), planes - plane, planes, axis=0
        )
        gate_all = gate_all.transpose(1, 0, 2).reshape(heads, width)

        part = width // n_tp
        mine = lax.dynamic_slice_in_dim(tokens, tp * part, part, axis=1)
        chunk = part // 2
        got = [
            over_tp(lax.ppermute(mine[:, c * chunk : (c + 1) * chunk], "seq", pair_swap))
            for c in (0, 1)
        ]
        partner_tokens = jnp.zeros_like(tokens)
        for i in range(n_tp):
            for c in (0, 1):
                partner_tokens = lax.dynamic_update_slice_in_dim(
                    partner_tokens, got[c][i], (tp ^ i) * part + c * chunk, axis=1
                )

        def pick(weight, parity):
            return lax.dynamic_slice_in_dim(weight, parity * hp * size, hp * size, axis=1)

        weights = {"q": query_weight, "k": key_weight, "v": value_weight}
        own = {n: pick(w, par) for n, w in weights.items()}
        other = {n: pick(w, 1 - par) for n, w in weights.items()}

        def gather(head, names):
            cut = slice(head * size, (head + 1) * size)
            keep = jnp.concatenate([own[n][:, cut] for n in names], axis=1)
            give = jnp.concatenate([other[n][:, cut] for n in names], axis=1)
            blocks = []
            for k in range(planes):
                one = keep if k == 0 else lax.ppermute(give if k % 2 else keep, "seq", from_plane(k))
                blocks += [one, lax.ppermute(one, "seq", half_swap)]
            return blocks

        gate_logit = lax.dot_general(
            tokens, gate_all, (((1,), (1,)), ((), ())), preferred_element_type=F32
        )
        log_decay = -decay_rate[None, :] * jax.nn.softplus(gate_logit)
        within_all = jnp.cumsum(log_decay, axis=0).T
        within_own = lax.dynamic_slice_in_dim(within_all, par * hp, hp, axis=0)
        within_partner = lax.ppermute(
            lax.dynamic_slice_in_dim(within_all, (1 - par) * hp, hp, axis=0), "seq", pair_swap
        )
        within = jnp.stack([within_own, within_partner])
        total = within[:, :, -1]
        wide = jnp.broadcast_to(within[..., None], within.shape + (size,))
        gain = lax.dynamic_slice_in_dim(norm_gain, par * hp * size, hp * size, axis=0)
        gain = gain.reshape(hp, 1, size)
        total_far = lax.ppermute(total, "seq", half_swap)

        def by_order(near, far):
            lo_near, hi_near = jnp.where(par == 0, near[0], near[1]), jnp.where(par == 0, near[1], near[0])
            lo_far, hi_far = jnp.where(par == 0, far[0], far[1]), jnp.where(par == 0, far[1], far[0])
            return (
                jnp.where(half == 0, lo_near, lo_far),
                jnp.where(half == 0, lo_far, lo_near),
                jnp.where(half == 0, hi_near, hi_far),
                jnp.where(half == 0, hi_far, hi_near),
            )

        toks = (tokens, partner_tokens)

        def states(head, keys, values):
            local = []
            for b in (0, 1):
                scale = jnp.exp(total[b, head] - wide[b, head])
                scaled = (scale * keys[b].astype(F32)).astype(BF)
                local.append(
                    lax.dot_general(
                        scaled, values[b], (((0,), (0,)), ((), ())), preferred_element_type=F32
                    )
                )
            local = jnp.stack(local)
            far = lax.ppermute(local, "seq", half_swap)
            s0, s1, s2, s3 = by_order(local, far)
            decays = jnp.exp(jnp.stack(by_order(total[:, head], total_far[:, head])))
            d0, d1, d2, d3 = decays[0], decays[1], decays[2], decays[3]
            quad = d3 * (d2 * (d1 * s0 + s1) + s2) + s3
            quad_decay = d0 * d1 * d2 * d3
            start = jnp.zeros_like(quad)
            for _ in range(n_seq // 4 - 1):
                start = lax.ppermute(quad_decay * start + quad, "seq", quad_up)
            p0 = start
            p1 = d0 * p0 + s0
            p2 = d1 * p1 + s1
            p3 = d2 * p2 + s2
            lo = jnp.where(half == 0, p0, p1).astype(BF)
            hi = jnp.where(half == 0, p2, p3).astype(BF)
            return jnp.where(par == 0, lo, hi), jnp.where(par == 0, hi, lo)

        def out_rows(head, i, other_parity):
            parity = 1 - par if other_parity else par
            start = ((tp ^ i) * heads + parity * hp + head) * size
            return lax.dynamic_slice_in_dim(out_weight, start, size, axis=0)

        mixed = None
        for head in range(hp):
            split = head == hp - 1
            groups = ("kv", "q") if split else ("kvq",)
            gathered = [gather(head, names) for names in groups]
            wide_out = [[project(where, toks[b], g, planes) for g in gathered] for b in (0, 1)]
            kvq = [jnp.concatenate(w, axis=1) if False else w for w in wide_out]

            def column(b, j):
                if split:
                    return kvq[b][1] if j == 2 else kvq[b][0][:, j * size : (j + 1) * size]
                return kvq[b][0][:, j * size : (j + 1) * size]

            keys, values, queries = ([column(b, j) for b in (0, 1)] for j in (0, 1, 2))
            prefix = states(head, keys, values)
            normed = [
                mix(
                    queries[b],
                    keys[b],
                    values[b],
                    wide[b, head],
                    within[b, head][None, :],
                    prefix[b],
                    gain[head],
                )
                for b in (1, 0)
            ][::-1]
            near = over_tp(normed[0])
            far = over_tp(lax.ppermute(normed[1], "seq", pair_swap))
            for flag, group in ((False, near), (True, far)):
                lhs = jnp.concatenate(group, axis=1)
                rhs = jnp.concatenate([out_rows(head, i, flag) for i in range(n_tp)], axis=0)
                piece = jnp.dot(lhs, rhs, preferred_element_type=F32)
                mixed = piece if mixed is None else mixed + piece
        return mixed.astype(BF)

    return jax.shard_map(
        on_device,
        mesh=mesh,
        in_specs=(
            P("seq", None),
            P("seq", "tp"),
            P("seq", "tp"),
            P("seq", "tp"),
            P("seq", "tp"),
            P("tp"),
            P("tp"),
            P(None, "tp"),
        ),
        out_specs=P("seq", "tp"),
        check_vma=False,
    )
```

```python
import functools

import jax
import jax.numpy as jnp
from jax import lax
from jax.experimental import pallas as pl
from jax.experimental.pallas import tpu as pltpu
from jax.sharding import PartitionSpec as P


BF = jnp.bfloat16
F32 = jnp.float32


def cost(flops, nbytes, trans=0):
    return pl.CostEstimate(flops=int(flops), bytes_accessed=int(nbytes), transcendentals=int(trans))


def params(mib):
    return pltpu.CompilerParams(vmem_limit_bytes=mib * 2**20)


VMEM = pl.BlockSpec(memory_space=pltpu.VMEM)


def call(kernel, out_shape, args, estimate, mib=14):
    return pl.pallas_call(
        kernel,
        out_shape=out_shape,
        in_specs=[VMEM] * len(args),
        compiler_params=params(mib),
        cost_estimate=estimate,
    )(*args)


def flag(flags_ref, row, shape):
    return jnp.broadcast_to(flags_ref[row : row + 1, 0:1], shape) > 0.5


def turn_kernel(where, tok_ref, *refs, planes, rows, other, tile):
    out_refs, sem = refs[:-1], refs[-1]
    plane = where[0] ^ other
    half = where[1]
    merged = rows % 128 != 0
    unit = 2 * rows if merged else rows
    copies = []
    for i in range(tok_ref.shape[1] // unit):
        if merged:
            block = lax.rem(plane + i, planes)
        else:
            block = lax.rem(plane + i // 2, planes) * 2 + (half if i % 2 == 0 else 1 - half)
        cols = pl.ds(pl.multiple_of(block * unit, unit), unit)
        first = pl.multiple_of(where[3] * tile, tile) if tile else 0
        for out_ref in out_refs:
            copies.append(
                pltpu.make_async_copy(
                    tok_ref.at[pl.ds(first, out_ref.shape[0]), cols],
                    out_ref.at[:, pl.ds(i * unit, unit)],
                    sem.at[len(copies)],
                )
            )
            copies[-1].start()
            first = first + out_ref.shape[0]
    for copy in copies:
        copy.wait()


def turn(where, tokens, planes, rows, tile, sizes, other, mib):
    width = tokens.shape[1]
    unit = 2 * rows if rows % 128 else rows
    return pl.pallas_call(
        functools.partial(turn_kernel, planes=planes, rows=rows, other=other, tile=tile),
        out_shape=[jax.ShapeDtypeStruct((size, width), BF) for size in sizes],
        in_specs=[
            pl.BlockSpec(memory_space=pltpu.SMEM),
            pl.BlockSpec(memory_space=pltpu.HBM),
        ],
        out_specs=[VMEM] * len(sizes),
        scratch_shapes=[pltpu.SemaphoreType.DMA((len(sizes) * width // unit,))],
        compiler_params=params(mib),
        cost_estimate=cost(1e6, 4 * sum(sizes) * width),
    )(where, tokens)


def pack_kernel(flags_ref, k_ref, v_ref, q_ref, *out_refs, groups, size, hp):
    refs = {"k": k_ref, "v": v_ref, "q": q_ref}
    odd = flag(flags_ref, 1, (k_ref.shape[0], size))
    for o, (head, names) in enumerate(groups):
        for j, n in enumerate(names):
            low = refs[n][:, head * size : (head + 1) * size]
            high = refs[n][:, (hp + head) * size : (hp + head + 1) * size]
            out_refs[2 * o][:, j * size : (j + 1) * size] = jnp.where(odd, high, low)
            out_refs[2 * o + 1][:, j * size : (j + 1) * size] = jnp.where(odd, low, high)


def decay_kernel(flags_ref, tok_ref, gate_ref, rate_ref, out_ref, *, hp):
    logit = lax.dot_general(
        gate_ref[...], tok_ref[...], (((1,), (1,)), ((), ())), preferred_element_type=F32
    )
    logit = logit[0 : rate_ref.shape[0], :]
    soft = jnp.maximum(logit, 0.0) + jnp.log1p(jnp.exp(-jnp.abs(logit)))
    run = -rate_ref[...] * soft
    lane = lax.broadcasted_iota(jnp.int32, run.shape, 1)
    step = 1
    while step < run.shape[1]:
        run = run + jnp.where(lane >= step, pltpu.roll(run, step, 1), 0.0)
        step *= 2
    odd = flag(flags_ref, 1, (hp, run.shape[1]))
    low, high = run[0:hp, :], run[hp : 2 * hp, :]
    out_ref[...] = jnp.zeros_like(out_ref)
    out_ref[0:hp, :] = jnp.where(odd, high, low)
    out_ref[hp : 2 * hp, :] = jnp.where(odd, low, high)


def project_kernel(flags_ref, *refs, parts, n_tp):
    tok_refs, block_refs, out_ref = refs[:parts], refs[parts:-1], refs[-1]
    rows = block_refs[0].shape[0]
    cols = out_ref.shape[1]
    tok_rows = out_ref.shape[0]
    tile = tok_rows // n_tp

    def product(pick):
        acc = None
        for i, block_ref in enumerate(block_refs):
            part = jnp.dot(
                pick(slice(i * rows, (i + 1) * rows)), block_ref[...], preferred_element_type=F32
            )
            acc = part if acc is None else acc + part
        return acc

    if parts == 1:
        big = 256 if tok_rows % 256 == 0 else tile
        for r in range(tok_rows // big):
            cut = slice(r * big, (r + 1) * big)
            out_ref[cut, :] = product(lambda at: tok_refs[0][cut, at]).astype(BF)
        return
    each = parts // n_tp
    got = []
    for r in range(0, n_tp, 2):
        acc = product(
            lambda at: jnp.concatenate([ref[:, at] for ref in tok_refs[r * each : (r + 2) * each]], axis=0)
        )
        got += [acc[:tile].astype(BF), acc[tile:].astype(BF)]
    bit, row = 1, 2
    while bit < n_tp:
        swap = flag(flags_ref, row, (tile, cols))
        got = [jnp.where(swap, got[i ^ bit], got[i]) for i in range(n_tp)]
        bit, row = 2 * bit, row + 1
    for i in range(n_tp):
        out_ref[i * tile : (i + 1) * tile, :] = got[i]


def project(flags, first, toks, blocks, n_tp):
    tok_rows = sum(t.shape[0] for t in toks)
    width, cols = toks[0].shape[1], blocks[0].shape[1]
    if blocks[0].shape[0] % 128:
        blocks = [
            jnp.concatenate([jnp.where(first, a, b), jnp.where(first, b, a)], axis=0)
            for a, b in zip(blocks[0::2], blocks[1::2])
        ]
    return call(
        functools.partial(project_kernel, parts=len(toks), n_tp=n_tp),
        jax.ShapeDtypeStruct((tok_rows, cols), BF),
        (flags, *toks, *blocks),
        cost(2 * tok_rows * width * max(cols, 256), 2 * tok_rows * width),
        16,
    )


def spread(row, size):
    return jnp.broadcast_to(row, (size, row.shape[1])).T


def state_kernel(own_ref, far_ref, win_ref, winp_ref, out_ref, *, head, hp, size):
    for b, (kv_ref, row) in enumerate(
        ((own_ref, win_ref[head : head + 1, :]), (far_ref, winp_ref[hp + head : hp + head + 1, :]))
    ):
        total = row[:, row.shape[1] - 1 :]
        key = kv_ref[:, 0:size].astype(F32)
        scaled = (spread(jnp.exp(total - row), size) * key).astype(BF)
        out_ref[b, 0:size, :] = lax.dot_general(
            scaled, kv_ref[:, size : 2 * size], (((0,), (0,)), ((), ())), preferred_element_type=F32
        )
        out_ref[b, size:, :] = jnp.broadcast_to(total, (8, size))


def in_order(flags_ref, near_ref, far_ref, size):
    second = flag(flags_ref, 0, near_ref.shape[1:])
    odd = flag(flags_ref, 1, near_ref.shape[1:])
    low, high = [], []
    for ref in (near_ref, far_ref):
        own, partner = ref[0], ref[1]
        low.append(jnp.where(odd, partner, own))
        high.append(jnp.where(odd, own, partner))
    both = []
    for near, far in (low, high):
        both += [jnp.where(second, far, near), jnp.where(second, near, far)]
    return [x[0:size, :] for x in both], [jnp.exp(x[size : size + 1, :]) for x in both]


def quad_kernel(flags_ref, near_ref, far_ref, *refs, size):
    (s0, s1, s2, s3), (d0, d1, d2, d3) = in_order(flags_ref, near_ref, far_ref, size)
    state = s0
    if len(refs) == 2:
        state = d0 * refs[0][...] + s0
    refs[-1][...] = d3 * (d2 * (d1 * state + s1) + s2) + s3


def mix_kernel(flags_ref, *refs, which, head, hp, size, tile, starts):
    kvq, refs = refs[: 2 * len(which)], refs[2 * len(which) :]
    windows, refs = refs[: len(which)], refs[len(which) :]
    near_ref, far_ref, gain_ref = refs[:3]
    out_refs = refs[-len(which) :]
    (s0, s1, s2, _), (d0, d1, d2, _) = in_order(flags_ref, near_ref, far_ref, size)
    p0 = refs[3][...] if starts else jnp.zeros_like(s0)
    p1 = d0 * p0 + s0
    p2 = d1 * p1 + s1
    p3 = d2 * p2 + s2
    second, odd = flag(flags_ref, 0, (size, size)), flag(flags_ref, 1, (size, size))
    low = jnp.where(second, p1, p0)
    high = jnp.where(second, p3, p2)
    gain = jnp.where(
        flag(flags_ref, 1, (1, size)),
        gain_ref[hp + head : hp + head + 1, :],
        gain_ref[head : head + 1, :],
    )
    for n, b in enumerate(which):
        kv_ref, q_ref = kvq[2 * n], kvq[2 * n + 1]
        q_at = q_ref.shape[1] - size
        state = (jnp.where(odd, low, high) if b else jnp.where(odd, high, low)).astype(BF)
        at = b * hp + head
        row = windows[n][at : at + 1, :]
        wide = spread(row, size)
        tok_rows = kv_ref.shape[0]
        for i in range(tok_rows // tile):
            lo, hi = i * tile, (i + 1) * tile
            query = q_ref[lo:hi, q_at:]
            wide_i = wide[lo:hi, :]
            scores = lax.dot_general(
                query, kv_ref[0:hi, 0:size], (((1,), (1,)), ((), ())), preferred_element_type=F32
            )
            gap = wide_i[:, 0:1] - row[:, 0:hi]
            row_index = lo + lax.broadcasted_iota(jnp.int32, (tile, hi), 0)
            col_index = lax.broadcasted_iota(jnp.int32, (tile, hi), 1)
            causal = col_index <= row_index
            attn = jnp.where(causal, scores * jnp.exp(jnp.where(causal, gap, 0.0)), 0.0).astype(BF)
            local = jnp.dot(attn, kv_ref[0:hi, size : 2 * size], preferred_element_type=F32)
            scaled = (jnp.exp(wide_i) * query.astype(F32)).astype(BF)
            carried = jnp.dot(scaled, state, preferred_element_type=F32)
            head_out = carried + local
            mean_square = jnp.mean(head_out * head_out, axis=-1, keepdims=True)
            normed = head_out * lax.rsqrt(mean_square + 1e-05) * gain
            out_refs[n][lo:hi, :] = normed.astype(BF)


def join_kernel(a_ref, b_ref, out_ref):
    out_ref[:, : a_ref.shape[1]] = a_ref[...]
    out_ref[:, a_ref.shape[1] :] = b_ref[...]


def out_kernel(flags_ref, weight_ref, *refs, n_tp, heads, hp, head, flags, size, acc):
    out_ref = refs[-1]
    normed = refs[: len(refs) - 1 - acc]
    cols = out_ref.shape[1]
    odd = flag(flags_ref, 1, (size, cols))
    pieces = []
    for other in flags:
        rows = []
        for t in range(n_tp):
            low = weight_ref[(t * heads + head) * size : (t * heads + head + 1) * size, :]
            at = t * heads + hp + head
            high = weight_ref[at * size : (at + 1) * size, :]
            rows.append(jnp.where(odd, low, high) if other else jnp.where(odd, high, low))
        bit, row = 1, 2
        while bit < n_tp:
            swap = flag(flags_ref, row, (size, cols))
            rows = [jnp.where(swap, rows[i ^ bit], rows[i]) for i in range(n_tp)]
            bit, row = 2 * bit, row + 1
        pieces += rows
    total = None
    wide = normed[0].shape[1] // size
    tok_rows = out_ref.shape[0]
    tile = 256 if tok_rows % 256 == 0 else tok_rows
    right = jnp.concatenate(pieces, axis=0)
    for r in range(tok_rows // tile):
        cut = slice(r * tile, (r + 1) * tile)
        left = [ref[cut, f * size : (f + 1) * size] for f in range(wide) for ref in normed]
        total = jnp.dot(jnp.concatenate(left, axis=1), right, preferred_element_type=F32)
        if acc:
            total = total + refs[-2][cut, :]
        out_ref[cut, :] = total.astype(out_ref.dtype)


def solution(mesh):
    n_seq, n_tp = mesh.shape["seq"], mesh.shape["tp"]
    planes = n_seq // 2
    hops = n_seq // 4 - 1
    bits = [1 << b for b in reversed(range((n_tp - 1).bit_length()))]
    steps = sorted(range(1, planes), key=lambda k: (k % 2 == 0, min(k, planes - k), k))

    def from_plane(step):
        return [(2 * ((z + step) % planes) + y, 2 * z + y) for z in range(planes) for y in (0, 1)]

    half_swap = [(s, s ^ 1) for s in range(n_seq)]
    pair_swap = [(s, s ^ 2) for s in range(n_seq)]
    quad_up = [(s, s + 4) for s in range(n_seq - 4)]

    def over_tp(own):
        got = {0: own}
        for bit in bits:
            swap = [(t, t ^ bit) for t in range(n_tp)]
            got.update({i ^ bit: lax.ppermute(v, "tp", swap) for i, v in list(got.items())})
        return [got[i] for i in range(n_tp)]

    def body(
        tokens, query_weight, key_weight, value_weight, gate_weight, decay_rate, norm_gain, out_weight
    ):
        tok_rows, width = tokens.shape
        heads = decay_rate.shape[0]
        hp = heads // 2
        size = query_weight.shape[1] // heads
        tp = lax.axis_index("tp")
        rank = lax.axis_index("seq")
        half = rank % 2
        plane = rank // 2
        par = plane % 2
        where = jnp.stack([plane, half, par, tp]).astype(jnp.int32)
        tp_bits = [(tp >> b) & 1 for b in range((n_tp - 1).bit_length())]
        flags = jnp.stack([half, par, *tp_bits] + [par] * (6 - len(tp_bits))).astype(F32)
        flags = jnp.broadcast_to(flags[:, None], (8, 128))
        groups = [(h, "kvq") for h in range(hp - 1)] + [(hp - 1, "kv"), (hp - 1, "q")]
        rows = key_weight.shape[0]

        tile = tok_rows // n_tp
        last = tile // 3 if tile % 48 == 0 else tile // 2
        sizes = (tile - last, last)
        chunks = len(sizes)
        mine = turn(where, tokens, planes, rows, tile, sizes, 1, 61)
        pieces = [None] * (n_tp * chunks)
        for c in range(chunks):
            got = over_tp(lax.ppermute(mine[c], "seq", pair_swap))
            for i in range(n_tp):
                pieces[i * chunks + c] = got[i]
        (own_tokens,) = turn(where, tokens, planes, rows, 0, (tok_rows,), 0, 52)

        packed = call(
            functools.partial(pack_kernel, groups=groups, size=size, hp=hp),
            [
                jax.ShapeDtypeStruct((rows, len(names) * size), BF)
                for _, names in groups
                for _ in (0, 1)
            ],
            (flags, key_weight, value_weight, query_weight),
            cost(1e6, key_weight.size * 12),
        )

        def gather(g):
            keep, give = packed[2 * g], packed[2 * g + 1]
            got = {0: keep}
            for k in steps:
                got[k] = lax.ppermute(give if k % 2 else keep, "seq", from_plane(k))
            blocks = []
            for k in range(planes):
                blocks += [got[k], lax.ppermute(got[k], "seq", half_swap)]
            return blocks

        gathered = [gather(g) for g in range(len(groups))]

        gate = gate_weight.T
        gate_z = {k: lax.ppermute(gate, "seq", from_plane(k)) for k in steps}
        gate_z = jnp.stack([gate] + [gate_z[k] for k in range(1, planes)])
        gate_zy = lax.ppermute(gate_z, "seq", half_swap)
        if rows % 128:
            gate_z, gate_zy = (
                jnp.where(half == 0, gate_z, gate_zy),
                jnp.where(half == 0, gate_zy, gate_z),
            )
        gate_all = jnp.concatenate([gate_z, gate_zy], axis=2)
        gate_all = gate_all.transpose(1, 0, 2).reshape(heads, width)
        rows8 = -(-heads // 8) * 8
        gate_all = jnp.pad(gate_all, ((0, 2 * rows8 - heads), (0, 0)))
        rate = jnp.pad(decay_rate[:, None], ((0, rows8 - heads), (0, 0)))
        within = call(
            functools.partial(decay_kernel, hp=hp),
            jax.ShapeDtypeStruct((rows8, tok_rows), F32),
            (flags, own_tokens, gate_all, rate),
            cost(64 * tok_rows * width, 2 * tok_rows * width),
        )
        within_far = lax.ppermute(within, "seq", pair_swap)
        gain = norm_gain.reshape(heads, size)

        own_proj, far_proj = [], []
        for blocks in gathered:
            far_proj.append(project(flags, half == 0, pieces, blocks, n_tp))
            own_proj.append(project(flags, half == 0, [own_tokens], blocks, n_tp))
        proj = list(zip(own_proj, far_proj))
        acc = []

        def out(normed, head, other, last):
            return call(
                functools.partial(
                    out_kernel,
                    n_tp=n_tp,
                    heads=heads,
                    hp=hp,
                    head=head,
                    flags=other,
                    size=size,
                    acc=len(acc),
                ),
                jax.ShapeDtypeStruct((tok_rows, out_weight.shape[1]), BF if last else F32),
                (flags, out_weight, *normed, *acc),
                cost(
                    2 * tok_rows * size * n_tp * len(other) * out_weight.shape[1],
                    2 * out_weight.size,
                ),
                20,
            )

        for head in range(hp):
            kv = proj[head]
            q = proj[-1] if head == hp - 1 else kv
            local = call(
                functools.partial(state_kernel, head=head, hp=hp, size=size),
                jax.ShapeDtypeStruct((2, size + 8, size), F32),
                (kv[0], kv[1], within, within_far),
                cost(4 * tok_rows * size * size, 16 * tok_rows * size),
            )
            far = lax.ppermute(local, "seq", half_swap)
            start = []
            for _ in range(hops):
                quad = call(
                    functools.partial(quad_kernel, size=size),
                    jax.ShapeDtypeStruct((size, size), F32),
                    (flags, local, far, *start),
                    cost(1e6, 40 * size * size),
                )
                start = [lax.ppermute(quad, "seq", quad_up)]

            def mix(which):
                kvq = [a for b in which for a in (kv[b], q[b])]
                windows = [(within, within_far)[b] for b in which]
                shape = jax.ShapeDtypeStruct((tok_rows, size), BF)
                return call(
                    functools.partial(
                        mix_kernel,
                        which=which,
                        head=head,
                        hp=hp,
                        size=size,
                        tile=256 if tok_rows % 256 == 0 else tok_rows,
                        starts=len(start),
                    ),
                    [shape] * len(which),
                    (flags, *kvq, *windows, local, far, gain, *start),
                    cost(
                        4 * tok_rows * tok_rows * size * len(which),
                        12 * tok_rows * size,
                        tok_rows * tok_rows,
                    ),
                )

            if head < hp - 1:
                normed, normed_far = mix((0, 1))
                back = lax.ppermute(normed_far, "seq", pair_swap)
                both = call(
                    join_kernel,
                    jax.ShapeDtypeStruct((tok_rows, 2 * size), BF),
                    (normed, back),
                    cost(1e6, 8 * tok_rows * size),
                )
                both = over_tp(both)
                acc = [out(both, head, (0, 1), False)]
            else:
                (normed_far,) = mix((1,))
                back = lax.ppermute(normed_far, "seq", pair_swap)
                (normed,) = mix((0,))
                acc = [out(over_tp(normed), head, (0,), False)]
                return out(over_tp(back), head, (1,), True)

    return jax.shard_map(
        body,
        mesh=mesh,
        in_specs=(
            P("seq", None),
            P("seq", "tp"),
            P("seq", "tp"),
            P("seq", "tp"),
            P("seq", "tp"),
            P("tp"),
            P("tp"),
            P(None, "tp"),
        ),
        out_specs=P("seq", "tp"),
        check_vma=False,
    )
```

```python
import functools

import jax
import jax.numpy as jnp
from jax import lax
from jax.experimental import pallas as pl
from jax.experimental.pallas import tpu as pltpu
from jax.sharding import PartitionSpec as P


BF = jnp.bfloat16
F32 = jnp.float32


def cost(flops, nbytes, trans=0):
    return pl.CostEstimate(flops=int(flops), bytes_accessed=int(nbytes), transcendentals=int(trans))


def params(mib):
    return pltpu.CompilerParams(vmem_limit_bytes=mib * 2**20)


VMEM = pl.BlockSpec(memory_space=pltpu.VMEM)


def call(kernel, out_shape, args, estimate, mib=14):
    return pl.pallas_call(
        kernel,
        out_shape=out_shape,
        in_specs=[VMEM] * len(args),
        compiler_params=params(mib),
        cost_estimate=estimate,
    )(*args)


def flag(flags_ref, row, shape):
    return jnp.broadcast_to(flags_ref[row : row + 1, 0:1], shape) > 0.5


def turn_kernel(where, tok_ref, *refs, planes, rows, other, tile):
    out_refs, sem = refs[:-1], refs[-1]
    plane = where[0] ^ other
    half = where[1]
    merged = rows % 128 != 0
    unit = 2 * rows if merged else rows
    copies = []
    for i in range(tok_ref.shape[1] // unit):
        if merged:
            block = lax.rem(plane + i, planes)
        else:
            block = lax.rem(plane + i // 2, planes) * 2 + (half if i % 2 == 0 else 1 - half)
        cols = pl.ds(pl.multiple_of(block * unit, unit), unit)
        first = pl.multiple_of(where[3] * tile, tile) if tile else 0
        for out_ref in out_refs:
            copies.append(
                pltpu.make_async_copy(
                    tok_ref.at[pl.ds(first, out_ref.shape[0]), cols],
                    out_ref.at[:, pl.ds(i * unit, unit)],
                    sem.at[len(copies)],
                )
            )
            copies[-1].start()
            first = first + out_ref.shape[0]
    for copy in copies:
        copy.wait()


def turn(where, tokens, planes, rows, tile, sizes, other, mib):
    width = tokens.shape[1]
    unit = 2 * rows if rows % 128 else rows
    return pl.pallas_call(
        functools.partial(turn_kernel, planes=planes, rows=rows, other=other, tile=tile),
        out_shape=[jax.ShapeDtypeStruct((size, width), BF) for size in sizes],
        in_specs=[
            pl.BlockSpec(memory_space=pltpu.SMEM),
            pl.BlockSpec(memory_space=pltpu.HBM),
        ],
        out_specs=[VMEM] * len(sizes),
        scratch_shapes=[pltpu.SemaphoreType.DMA((len(sizes) * width // unit,))],
        compiler_params=params(mib),
        cost_estimate=cost(1e6, 4 * sum(sizes) * width),
    )(where, tokens)


def pack_kernel(flags_ref, k_ref, v_ref, q_ref, *out_refs, groups, size, hp):
    refs = {"k": k_ref, "v": v_ref, "q": q_ref}
    odd = flag(flags_ref, 1, (k_ref.shape[0], size))
    for o, (head, names) in enumerate(groups):
        for j, n in enumerate(names):
            low = refs[n][:, head * size : (head + 1) * size]
            high = refs[n][:, (hp + head) * size : (hp + head + 1) * size]
            out_refs[2 * o][:, j * size : (j + 1) * size] = jnp.where(odd, high, low)
            out_refs[2 * o + 1][:, j * size : (j + 1) * size] = jnp.where(odd, low, high)


def decay_kernel(flags_ref, tok_ref, gate_ref, far_ref, rate_ref, out_ref, *, hp):
    heads = gate_ref.shape[1]
    gates = [ref[k] for k in range(gate_ref.shape[0]) for ref in (gate_ref, far_ref)]
    gate = jnp.concatenate(gates, axis=1).astype(F32)
    gate = jnp.concatenate([gate, jnp.zeros((16 - heads, gate.shape[1]), F32)], axis=0).astype(BF)
    logit = lax.dot_general(
        gate, tok_ref[...], (((1,), (1,)), ((), ())), preferred_element_type=F32
    )
    logit = logit[0:8, :]
    soft = jnp.maximum(logit, 0.0) + jnp.log1p(jnp.exp(-jnp.abs(logit)))
    run = -rate_ref[:, 0:1] * soft
    lane = lax.broadcasted_iota(jnp.int32, run.shape, 1)
    step = 1
    while step < run.shape[1]:
        run = run + jnp.where(lane >= step, pltpu.roll(run, step, 1), 0.0)
        step *= 2
    odd = flag(flags_ref, 1, (hp, run.shape[1]))
    low, high = run[0:hp, :], run[hp : 2 * hp, :]
    out_ref[...] = jnp.zeros_like(out_ref)
    out_ref[0:hp, :] = jnp.where(odd, high, low)
    out_ref[hp : 2 * hp, :] = jnp.where(odd, low, high)


def project_kernel(flags_ref, *refs, parts, n_tp):
    tok_refs, block_refs, out_ref = refs[:parts], refs[parts:-1], refs[-1]
    rows = block_refs[0].shape[0]
    cols = out_ref.shape[1]
    tok_rows = out_ref.shape[0]
    tile = tok_rows // n_tp

    def product(pick):
        acc = None
        for i, block_ref in enumerate(block_refs):
            part = jnp.dot(
                pick(slice(i * rows, (i + 1) * rows)), block_ref[...], preferred_element_type=F32
            )
            acc = part if acc is None else acc + part
        return acc

    if parts == 1:
        big = 256 if tok_rows % 256 == 0 else tile
        for r in range(tok_rows // big):
            cut = slice(r * big, (r + 1) * big)
            out_ref[cut, :] = product(lambda at: tok_refs[0][cut, at]).astype(BF)
        return
    each = parts // n_tp
    got = []
    for r in range(0, n_tp, 2):
        acc = product(
            lambda at: jnp.concatenate([ref[:, at] for ref in tok_refs[r * each : (r + 2) * each]], axis=0)
        )
        got += [acc[:tile].astype(BF), acc[tile:].astype(BF)]
    bit, row = 1, 2
    while bit < n_tp:
        swap = flag(flags_ref, row, (tile, cols))
        got = [jnp.where(swap, got[i ^ bit], got[i]) for i in range(n_tp)]
        bit, row = 2 * bit, row + 1
    for i in range(n_tp):
        out_ref[i * tile : (i + 1) * tile, :] = got[i]


def project(flags, first, toks, blocks, n_tp):
    tok_rows = sum(t.shape[0] for t in toks)
    width, cols = toks[0].shape[1], blocks[0].shape[1]
    if blocks[0].shape[0] % 128:
        blocks = [
            jnp.concatenate([jnp.where(first, a, b), jnp.where(first, b, a)], axis=0)
            for a, b in zip(blocks[0::2], blocks[1::2])
        ]
    return call(
        functools.partial(project_kernel, parts=len(toks), n_tp=n_tp),
        jax.ShapeDtypeStruct((tok_rows, cols), BF),
        (flags, *toks, *blocks),
        cost(2 * tok_rows * width * max(cols, 256), 2 * tok_rows * width),
        16,
    )


def spread(row, size):
    return jnp.broadcast_to(row, (size, row.shape[1])).T


def state_kernel(own_ref, far_ref, win_ref, winp_ref, out_ref, *, head, hp, size):
    for b, (kv_ref, row) in enumerate(
        ((own_ref, win_ref[head : head + 1, :]), (far_ref, winp_ref[hp + head : hp + head + 1, :]))
    ):
        total = row[:, row.shape[1] - 1 :]
        key = kv_ref[:, 0:size].astype(F32)
        scaled = (spread(jnp.exp(total - row), size) * key).astype(BF)
        out_ref[b, 0:size, :] = lax.dot_general(
            scaled, kv_ref[:, size : 2 * size], (((0,), (0,)), ((), ())), preferred_element_type=F32
        )
        out_ref[b, size:, :] = jnp.broadcast_to(total, (8, size))


def in_order(flags_ref, near_ref, far_ref, size):
    second = flag(flags_ref, 0, near_ref.shape[1:])
    odd = flag(flags_ref, 1, near_ref.shape[1:])
    low, high = [], []
    for ref in (near_ref, far_ref):
        own, partner = ref[0], ref[1]
        low.append(jnp.where(odd, partner, own))
        high.append(jnp.where(odd, own, partner))
    both = []
    for near, far in (low, high):
        both += [jnp.where(second, far, near), jnp.where(second, near, far)]
    return [x[0:size, :] for x in both], [jnp.exp(x[size : size + 1, :]) for x in both]


def quad_kernel(flags_ref, near_ref, far_ref, *refs, size):
    (s0, s1, s2, s3), (d0, d1, d2, d3) = in_order(flags_ref, near_ref, far_ref, size)
    state = s0
    if len(refs) == 2:
        state = d0 * refs[0][...] + s0
    refs[-1][...] = d3 * (d2 * (d1 * state + s1) + s2) + s3


def mix_kernel(flags_ref, *refs, which, head, hp, size, tile, starts):
    kvq, refs = refs[: 2 * len(which)], refs[2 * len(which) :]
    windows, refs = refs[: len(which)], refs[len(which) :]
    near_ref, far_ref, gain_ref = refs[:3]
    out_refs = refs[-len(which) :]
    (s0, s1, s2, _), (d0, d1, d2, _) = in_order(flags_ref, near_ref, far_ref, size)
    p0 = refs[3][...] if starts else jnp.zeros_like(s0)
    p1 = d0 * p0 + s0
    p2 = d1 * p1 + s1
    p3 = d2 * p2 + s2
    second, odd = flag(flags_ref, 0, (size, size)), flag(flags_ref, 1, (size, size))
    low = jnp.where(second, p1, p0)
    high = jnp.where(second, p3, p2)
    gain = jnp.where(
        flag(flags_ref, 1, (1, size)),
        gain_ref[hp + head : hp + head + 1, :],
        gain_ref[head : head + 1, :],
    )
    for n, b in enumerate(which):
        kv_ref, q_ref = kvq[2 * n], kvq[2 * n + 1]
        q_at = q_ref.shape[1] - size
        state = (jnp.where(odd, low, high) if b else jnp.where(odd, high, low)).astype(BF)
        at = b * hp + head
        row = windows[n][at : at + 1, :]
        wide = spread(row, size)
        tok_rows = kv_ref.shape[0]
        for i in range(tok_rows // tile):
            lo, hi = i * tile, (i + 1) * tile
            query = q_ref[lo:hi, q_at:]
            wide_i = wide[lo:hi, :]
            scores = lax.dot_general(
                query, kv_ref[0:hi, 0:size], (((1,), (1,)), ((), ())), preferred_element_type=F32
            )
            gap = wide_i[:, 0:1] - row[:, 0:hi]
            row_index = lo + lax.broadcasted_iota(jnp.int32, (tile, hi), 0)
            col_index = lax.broadcasted_iota(jnp.int32, (tile, hi), 1)
            causal = col_index <= row_index
            attn = jnp.where(causal, scores * jnp.exp(jnp.where(causal, gap, 0.0)), 0.0).astype(BF)
            local = jnp.dot(attn, kv_ref[0:hi, size : 2 * size], preferred_element_type=F32)
            scaled = (jnp.exp(wide_i) * query.astype(F32)).astype(BF)
            carried = jnp.dot(scaled, state, preferred_element_type=F32)
            head_out = carried + local
            mean_square = jnp.mean(head_out * head_out, axis=-1, keepdims=True)
            normed = head_out * lax.rsqrt(mean_square + 1e-05) * gain
            out_refs[n][lo:hi, :] = normed.astype(BF)


def out_kernel(flags_ref, weight_ref, *refs, n_tp, heads, hp, head, flags, size, acc):
    out_ref = refs[-1]
    normed = refs[: len(refs) - 1 - acc]
    cols = out_ref.shape[1]
    odd = flag(flags_ref, 1, (size, cols))
    pieces = []
    for other in flags:
        rows = []
        for t in range(n_tp):
            low = weight_ref[(t * heads + head) * size : (t * heads + head + 1) * size, :]
            at = t * heads + hp + head
            high = weight_ref[at * size : (at + 1) * size, :]
            rows.append(jnp.where(odd, low, high) if other else jnp.where(odd, high, low))
        bit, row = 1, 2
        while bit < n_tp:
            swap = flag(flags_ref, row, (size, cols))
            rows = [jnp.where(swap, rows[i ^ bit], rows[i]) for i in range(n_tp)]
            bit, row = 2 * bit, row + 1
        pieces += rows
    total = None
    wide = normed[0].shape[1] // size
    tok_rows = out_ref.shape[0]
    tile = 256 if tok_rows % 256 == 0 else tok_rows
    right = jnp.concatenate(pieces, axis=0)
    for r in range(tok_rows // tile):
        cut = slice(r * tile, (r + 1) * tile)
        left = [ref[cut, f * size : (f + 1) * size] for f in range(wide) for ref in normed]
        total = jnp.dot(jnp.concatenate(left, axis=1), right, preferred_element_type=F32)
        if acc:
            total = total + refs[-2][cut, :]
        out_ref[cut, :] = total.astype(out_ref.dtype)


def solution(mesh):
    n_seq, n_tp = mesh.shape["seq"], mesh.shape["tp"]
    planes = n_seq // 2
    hops = n_seq // 4 - 1
    chunks = 3
    bits = [1 << b for b in reversed(range((n_tp - 1).bit_length()))]
    steps = sorted(range(1, planes), key=lambda k: (k % 2 == 0, min(k, planes - k), k))

    def from_plane(step):
        return [(2 * ((z + step) % planes) + y, 2 * z + y) for z in range(planes) for y in (0, 1)]

    half_swap = [(s, s ^ 1) for s in range(n_seq)]
    pair_swap = [(s, s ^ 2) for s in range(n_seq)]
    quad_up = [(s, s + 4) for s in range(n_seq - 4)]

    def over_tp(own):
        got = {0: own}
        for bit in bits:
            swap = [(t, t ^ bit) for t in range(n_tp)]
            got.update({i ^ bit: lax.ppermute(v, "tp", swap) for i, v in list(got.items())})
        return [got[i] for i in range(n_tp)]

    def body(
        tokens, query_weight, key_weight, value_weight, gate_weight, decay_rate, norm_gain, out_weight
    ):
        tok_rows, width = tokens.shape
        heads = decay_rate.shape[0]
        hp = heads // 2
        size = query_weight.shape[1] // heads
        tp = lax.axis_index("tp")
        rank = lax.axis_index("seq")
        half = rank % 2
        plane = rank // 2
        par = plane % 2
        where = jnp.stack([plane, half, par, tp]).astype(jnp.int32)
        tp_bits = [(tp >> b) & 1 for b in range((n_tp - 1).bit_length())]
        flags = jnp.stack([half, par, *tp_bits] + [par] * (6 - len(tp_bits))).astype(F32)
        flags = jnp.broadcast_to(flags[:, None], (8, 128))
        groups = [(h, "kvq") for h in range(hp - 1)] + [(hp - 1, "kv"), (hp - 1, "q")]
        rows = key_weight.shape[0]

        tile = tok_rows // n_tp
        sizes = (tile // chunks,) * chunks
        mine = turn(where, tokens, planes, rows, tile, sizes, 1, 61)
        pieces = [None] * (n_tp * chunks)
        for c in range(chunks):
            got = over_tp(lax.ppermute(mine[c], "seq", pair_swap))
            for i in range(n_tp):
                pieces[i * chunks + c] = got[i]
        (own_tokens,) = turn(where, tokens, planes, rows, 0, (tok_rows,), 0, 52)

        packed = call(
            functools.partial(pack_kernel, groups=groups, size=size, hp=hp),
            [
                jax.ShapeDtypeStruct((rows, len(names) * size), BF)
                for _, names in groups
                for _ in (0, 1)
            ],
            (flags, key_weight, value_weight, query_weight),
            cost(1e6, key_weight.size * 12),
            61,
        )

        def gather(g):
            keep, give = packed[2 * g], packed[2 * g + 1]
            got = {0: keep}
            for k in steps:
                got[k] = lax.ppermute(give if k % 2 else keep, "seq", from_plane(k))
            blocks = []
            for k in range(planes):
                blocks += [got[k], lax.ppermute(got[k], "seq", half_swap)]
            return blocks

        gathered = [gather(g) for g in range(len(groups))]

        gate = gate_weight.T
        gate_z = {k: lax.ppermute(gate, "seq", from_plane(k)) for k in steps}
        gate_z = jnp.stack([gate] + [gate_z[k] for k in range(1, planes)])
        gate_zy = lax.ppermute(gate_z, "seq", half_swap)
        if rows % 128:
            gate_z, gate_zy = (
                jnp.where(half == 0, gate_z, gate_zy),
                jnp.where(half == 0, gate_zy, gate_z),
            )
        rate = jnp.broadcast_to(jnp.pad(decay_rate, (0, 8 - heads))[:, None], (8, 128))
        within = call(
            functools.partial(decay_kernel, hp=hp),
            jax.ShapeDtypeStruct((8, tok_rows), F32),
            (flags, own_tokens, gate_z, gate_zy, rate),
            cost(64 * tok_rows * width, 2 * tok_rows * width),
        )
        within_far = lax.ppermute(within, "seq", pair_swap)
        gain = norm_gain.reshape(heads, size)

        own_proj, far_proj = [], []
        for blocks in gathered:
            far_proj.append(project(flags, half == 0, pieces, blocks, n_tp))
            own_proj.append(project(flags, half == 0, [own_tokens], blocks, n_tp))
        proj = list(zip(own_proj, far_proj))
        acc = []

        def out(normed, head, other, last):
            return call(
                functools.partial(
                    out_kernel,
                    n_tp=n_tp,
                    heads=heads,
                    hp=hp,
                    head=head,
                    flags=other,
                    size=size,
                    acc=len(acc),
                ),
                jax.ShapeDtypeStruct((tok_rows, out_weight.shape[1]), BF if last else F32),
                (flags, out_weight, *normed, *acc),
                cost(
                    2 * tok_rows * size * n_tp * len(other) * out_weight.shape[1],
                    2 * out_weight.size,
                ),
                20,
            )

        for head in range(hp):
            kv = proj[head]
            q = proj[-1] if head == hp - 1 else kv
            local = call(
                functools.partial(state_kernel, head=head, hp=hp, size=size),
                jax.ShapeDtypeStruct((2, size + 8, size), F32),
                (kv[0], kv[1], within, within_far),
                cost(4 * tok_rows * size * size, 16 * tok_rows * size),
            )
            far = lax.ppermute(local, "seq", half_swap)
            start = []
            for _ in range(hops):
                quad = call(
                    functools.partial(quad_kernel, size=size),
                    jax.ShapeDtypeStruct((size, size), F32),
                    (flags, local, far, *start),
                    cost(1e6, 40 * size * size),
                )
                start = [lax.ppermute(quad, "seq", quad_up)]

            def mix(which):
                kvq = [a for b in which for a in (kv[b], q[b])]
                windows = [(within, within_far)[b] for b in which]
                shape = jax.ShapeDtypeStruct((tok_rows, size), BF)
                return call(
                    functools.partial(
                        mix_kernel,
                        which=which,
                        head=head,
                        hp=hp,
                        size=size,
                        tile=256 if tok_rows % 256 == 0 else tok_rows,
                        starts=len(start),
                    ),
                    [shape] * len(which),
                    (flags, *kvq, *windows, local, far, gain, *start),
                    cost(
                        4 * tok_rows * tok_rows * size * len(which),
                        12 * tok_rows * size,
                        tok_rows * tok_rows,
                    ),
                )

            if head < hp - 1:
                normed, normed_far = mix((0, 1))
                back = lax.ppermute(normed_far, "seq", pair_swap)
                both = over_tp(normed) + over_tp(back)
                acc = [out(both, head, (0, 1), False)]
            else:
                (normed_far,) = mix((1,))
                back = lax.ppermute(normed_far, "seq", pair_swap)
                (normed,) = mix((0,))
                acc = [out(over_tp(normed), head, (0,), False)]
                return out(over_tp(back), head, (1,), True)

    return jax.shard_map(
        body,
        mesh=mesh,
        in_specs=(
            P("seq", None),
            P("seq", "tp"),
            P("seq", "tp"),
            P("seq", "tp"),
            P("seq", "tp"),
            P("tp"),
            P("tp"),
            P(None, "tp"),
        ),
        out_specs=P("seq", "tp"),
        check_vma=False,
    )
```

```python
import functools

import jax
import jax.numpy as jnp
from jax import lax
from jax.experimental import pallas as pl
from jax.experimental.pallas import tpu as pltpu
from jax.sharding import PartitionSpec as P


BF = jnp.bfloat16
F32 = jnp.float32


def cost(flops, nbytes, trans=0):
    return pl.CostEstimate(flops=int(flops), bytes_accessed=int(nbytes), transcendentals=int(trans))


def params(mib):
    return pltpu.CompilerParams(vmem_limit_bytes=mib * 2**20)


VMEM = pl.BlockSpec(memory_space=pltpu.VMEM)


def call(kernel, out_shape, args, estimate, mib=14):
    return pl.pallas_call(
        kernel,
        out_shape=out_shape,
        in_specs=[VMEM] * len(args),
        compiler_params=params(mib),
        cost_estimate=estimate,
    )(*args)


def flag(flags_ref, row, shape):
    return jnp.broadcast_to(flags_ref[row : row + 1, 0:1], shape) > 0.5


def turn_kernel(where, tok_ref, *refs, planes, rows, other, tile):
    out_refs, sem = refs[:-1], refs[-1]
    plane = where[0] ^ other
    half = where[1]
    merged = rows % 128 != 0
    unit = 2 * rows if merged else rows
    copies = []
    for i in range(tok_ref.shape[1] // unit):
        if merged:
            block = lax.rem(plane + i, planes)
        else:
            block = lax.rem(plane + i // 2, planes) * 2 + (half if i % 2 == 0 else 1 - half)
        cols = pl.ds(pl.multiple_of(block * unit, unit), unit)
        first = pl.multiple_of(where[3] * tile, tile) if tile else 0
        for out_ref in out_refs:
            copies.append(
                pltpu.make_async_copy(
                    tok_ref.at[pl.ds(first, out_ref.shape[0]), cols],
                    out_ref.at[:, pl.ds(i * unit, unit)],
                    sem.at[len(copies)],
                )
            )
            copies[-1].start()
            first = first + out_ref.shape[0]
    for copy in copies:
        copy.wait()


def turn(where, tokens, planes, rows, tile, sizes, other, mib):
    width = tokens.shape[1]
    unit = 2 * rows if rows % 128 else rows
    return pl.pallas_call(
        functools.partial(turn_kernel, planes=planes, rows=rows, other=other, tile=tile),
        out_shape=[jax.ShapeDtypeStruct((size, width), BF) for size in sizes],
        in_specs=[
            pl.BlockSpec(memory_space=pltpu.SMEM),
            pl.BlockSpec(memory_space=pltpu.HBM),
        ],
        out_specs=[VMEM] * len(sizes),
        scratch_shapes=[pltpu.SemaphoreType.DMA((len(sizes) * width // unit,))],
        compiler_params=params(mib),
        cost_estimate=cost(1e6, 4 * sum(sizes) * width),
    )(where, tokens)


def gate_rows(rows):
    wide = min(rows, 256)
    return rows // wide, wide


def pack_kernel(flags_ref, k_ref, v_ref, q_ref, gate_ref, *out_refs, groups, size, hp):
    rows = k_ref.shape[0]
    parts, wide = gate_rows(rows)
    gate = gate_ref[...].astype(F32)
    tail = jnp.concatenate([gate[:, p * wide : (p + 1) * wide] for p in range(parts)], axis=0)
    below = out_refs[0].shape[0] - rows
    if tail.shape[0] < below:
        tail = jnp.concatenate([tail, jnp.zeros((below - tail.shape[0], wide), F32)], axis=0)
    for out_ref in out_refs[:2]:
        rest = out_ref.shape[1] - wide
        out_ref[rows:, :] = jnp.concatenate([tail, jnp.zeros((below, rest), F32)], axis=1).astype(BF)
    refs = {"k": k_ref, "v": v_ref, "q": q_ref}
    odd = flag(flags_ref, 1, (rows, size))
    for o, (head, names) in enumerate(groups):
        for j, n in enumerate(names):
            low = refs[n][:, head * size : (head + 1) * size]
            high = refs[n][:, (hp + head) * size : (hp + head + 1) * size]
            out_refs[2 * o][0:rows, j * size : (j + 1) * size] = jnp.where(odd, high, low)
            out_refs[2 * o + 1][0:rows, j * size : (j + 1) * size] = jnp.where(odd, low, high)


def decay_kernel(flags_ref, tok_ref, rate_ref, *refs, hp, rows):
    block_refs, out_ref = refs[:-1], refs[-1]
    heads = 2 * hp
    parts, wide = gate_rows(rows)
    gates = []
    for block_ref in block_refs:
        tail = block_ref[rows:, 0:wide].astype(F32)
        gates.append(
            jnp.concatenate([tail[p * heads : (p + 1) * heads] for p in range(parts)], axis=1)
        )
    if rows % 128:
        second = flag(flags_ref, 0, gates[0].shape)
        for i in range(0, len(gates), 2):
            a, b = gates[i], gates[i + 1]
            gates[i], gates[i + 1] = jnp.where(second, b, a), jnp.where(second, a, b)
    gate = jnp.concatenate(gates, axis=1)
    gate = jnp.concatenate([gate, jnp.zeros((16 - heads, gate.shape[1]), F32)], axis=0).astype(BF)
    logit = lax.dot_general(
        gate, tok_ref[...], (((1,), (1,)), ((), ())), preferred_element_type=F32
    )
    logit = logit[0:8, :]
    soft = jnp.maximum(logit, 0.0) + jnp.log1p(jnp.exp(-jnp.abs(logit)))
    run = -rate_ref[:, 0:1] * soft
    lane = lax.broadcasted_iota(jnp.int32, run.shape, 1)
    step = 1
    while step < run.shape[1]:
        run = run + jnp.where(lane >= step, pltpu.roll(run, step, 1), 0.0)
        step *= 2
    odd = flag(flags_ref, 1, (hp, run.shape[1]))
    low, high = run[0:hp, :], run[hp : 2 * hp, :]
    out_ref[...] = jnp.zeros_like(out_ref)
    out_ref[0:hp, :] = jnp.where(odd, high, low)
    out_ref[hp : 2 * hp, :] = jnp.where(odd, low, high)


def project_kernel(flags_ref, *refs, parts, n_tp, rows):
    tok_refs, block_refs, out_ref = refs[:parts], refs[parts:-1], refs[-1]
    cols = out_ref.shape[1]
    tok_rows = out_ref.shape[0]
    tile = tok_rows // n_tp

    def product(pick):
        acc = None
        for i, block_ref in enumerate(block_refs):
            part = jnp.dot(
                pick(slice(i * rows, (i + 1) * rows)),
                block_ref[0:rows, :],
                preferred_element_type=F32,
            )
            acc = part if acc is None else acc + part
        return acc

    if parts == 1:
        big = 256 if tok_rows % 256 == 0 else tile
        for r in range(tok_rows // big):
            cut = slice(r * big, (r + 1) * big)
            out_ref[cut, :] = product(lambda at: tok_refs[0][cut, at]).astype(BF)
        return
    each = parts // n_tp
    got = []
    for r in range(0, n_tp, 2):
        acc = product(
            lambda at: jnp.concatenate([ref[:, at] for ref in tok_refs[r * each : (r + 2) * each]], axis=0)
        )
        got += [acc[:tile].astype(BF), acc[tile:].astype(BF)]
    bit, row = 1, 2
    while bit < n_tp:
        swap = flag(flags_ref, row, (tile, cols))
        got = [jnp.where(swap, got[i ^ bit], got[i]) for i in range(n_tp)]
        bit, row = 2 * bit, row + 1
    for i in range(n_tp):
        out_ref[i * tile : (i + 1) * tile, :] = got[i]


def project(flags, first, toks, blocks, n_tp):
    tok_rows = sum(t.shape[0] for t in toks)
    width, cols = toks[0].shape[1], blocks[0].shape[1]
    rows = width // len(blocks)
    if rows % 128:
        blocks = [b[:rows] for b in blocks]
        blocks = [
            jnp.concatenate([jnp.where(first, a, b), jnp.where(first, b, a)], axis=0)
            for a, b in zip(blocks[0::2], blocks[1::2])
        ]
        rows = 2 * rows
    return call(
        functools.partial(project_kernel, parts=len(toks), n_tp=n_tp, rows=rows),
        jax.ShapeDtypeStruct((tok_rows, cols), BF),
        (flags, *toks, *blocks),
        cost(2 * tok_rows * width * max(cols, 256), 2 * tok_rows * width),
        16,
    )


def spread(row, size):
    return jnp.broadcast_to(row, (size, row.shape[1])).T


def state_kernel(own_ref, far_ref, win_ref, winp_ref, out_ref, *, head, hp, size):
    for b, (kv_ref, row) in enumerate(
        ((own_ref, win_ref[head : head + 1, :]), (far_ref, winp_ref[hp + head : hp + head + 1, :]))
    ):
        total = row[:, row.shape[1] - 1 :]
        key = kv_ref[:, 0:size].astype(F32)
        scaled = (spread(jnp.exp(total - row), size) * key).astype(BF)
        out_ref[b, 0:size, :] = lax.dot_general(
            scaled, kv_ref[:, size : 2 * size], (((0,), (0,)), ((), ())), preferred_element_type=F32
        )
        out_ref[b, size:, :] = jnp.broadcast_to(total, (8, size))


def in_order(flags_ref, near_ref, far_ref, size):
    second = flag(flags_ref, 0, near_ref.shape[1:])
    odd = flag(flags_ref, 1, near_ref.shape[1:])
    low, high = [], []
    for ref in (near_ref, far_ref):
        own, partner = ref[0], ref[1]
        low.append(jnp.where(odd, partner, own))
        high.append(jnp.where(odd, own, partner))
    both = []
    for near, far in (low, high):
        both += [jnp.where(second, far, near), jnp.where(second, near, far)]
    return [x[0:size, :] for x in both], [jnp.exp(x[size : size + 1, :]) for x in both]


def quad_kernel(flags_ref, near_ref, far_ref, *refs, size):
    (s0, s1, s2, s3), (d0, d1, d2, d3) = in_order(flags_ref, near_ref, far_ref, size)
    state = s0
    if len(refs) == 2:
        state = d0 * refs[0][...] + s0
    refs[-1][...] = d3 * (d2 * (d1 * state + s1) + s2) + s3


def mix_kernel(flags_ref, *refs, which, head, hp, size, tile, starts):
    kvq, refs = refs[: 2 * len(which)], refs[2 * len(which) :]
    windows, refs = refs[: len(which)], refs[len(which) :]
    near_ref, far_ref, gain_ref = refs[:3]
    out_refs = refs[-len(which) :]
    (s0, s1, s2, _), (d0, d1, d2, _) = in_order(flags_ref, near_ref, far_ref, size)
    p0 = refs[3][...] if starts else jnp.zeros_like(s0)
    p1 = d0 * p0 + s0
    p2 = d1 * p1 + s1
    p3 = d2 * p2 + s2
    second, odd = flag(flags_ref, 0, (size, size)), flag(flags_ref, 1, (size, size))
    low = jnp.where(second, p1, p0)
    high = jnp.where(second, p3, p2)
    gain = jnp.where(
        flag(flags_ref, 1, (1, size)),
        gain_ref[hp + head : hp + head + 1, :],
        gain_ref[head : head + 1, :],
    )
    for n, b in enumerate(which):
        kv_ref, q_ref = kvq[2 * n], kvq[2 * n + 1]
        q_at = q_ref.shape[1] - size
        state = (jnp.where(odd, low, high) if b else jnp.where(odd, high, low)).astype(BF)
        at = b * hp + head
        row = windows[n][at : at + 1, :]
        wide = spread(row, size)
        tok_rows = kv_ref.shape[0]
        for i in range(tok_rows // tile):
            lo, hi = i * tile, (i + 1) * tile
            query = q_ref[lo:hi, q_at:]
            wide_i = wide[lo:hi, :]
            scores = lax.dot_general(
                query, kv_ref[0:hi, 0:size], (((1,), (1,)), ((), ())), preferred_element_type=F32
            )
            gap = wide_i[:, 0:1] - row[:, 0:hi]
            row_index = lo + lax.broadcasted_iota(jnp.int32, (tile, hi), 0)
            col_index = lax.broadcasted_iota(jnp.int32, (tile, hi), 1)
            causal = col_index <= row_index
            attn = jnp.where(causal, scores * jnp.exp(jnp.where(causal, gap, 0.0)), 0.0).astype(BF)
            local = jnp.dot(attn, kv_ref[0:hi, size : 2 * size], preferred_element_type=F32)
            scaled = (jnp.exp(wide_i) * query.astype(F32)).astype(BF)
            carried = jnp.dot(scaled, state, preferred_element_type=F32)
            head_out = carried + local
            mean_square = jnp.mean(head_out * head_out, axis=-1, keepdims=True)
            normed = head_out * lax.rsqrt(mean_square + 1e-05) * gain
            out_refs[n][lo:hi, :] = normed.astype(BF)


def out_kernel(flags_ref, weight_ref, *refs, n_tp, heads, hp, head, flags, size, acc):
    out_ref = refs[-1]
    normed = refs[: len(refs) - 1 - acc]
    cols = out_ref.shape[1]
    odd = flag(flags_ref, 1, (size, cols))
    pieces = []
    for other in flags:
        rows = []
        for t in range(n_tp):
            low = weight_ref[(t * heads + head) * size : (t * heads + head + 1) * size, :]
            at = t * heads + hp + head
            high = weight_ref[at * size : (at + 1) * size, :]
            rows.append(jnp.where(odd, low, high) if other else jnp.where(odd, high, low))
        bit, row = 1, 2
        while bit < n_tp:
            swap = flag(flags_ref, row, (size, cols))
            rows = [jnp.where(swap, rows[i ^ bit], rows[i]) for i in range(n_tp)]
            bit, row = 2 * bit, row + 1
        pieces += rows
    total = None
    wide = normed[0].shape[1] // size
    tok_rows = out_ref.shape[0]
    tile = 256 if tok_rows % 256 == 0 else tok_rows
    right = jnp.concatenate(pieces, axis=0)
    for r in range(tok_rows // tile):
        cut = slice(r * tile, (r + 1) * tile)
        left = [ref[cut, f * size : (f + 1) * size] for f in range(wide) for ref in normed]
        total = jnp.dot(jnp.concatenate(left, axis=1), right, preferred_element_type=F32)
        if acc:
            total = total + refs[-2][cut, :]
        out_ref[cut, :] = total.astype(out_ref.dtype)


def solution(mesh):
    n_seq, n_tp = mesh.shape["seq"], mesh.shape["tp"]
    planes = n_seq // 2
    hops = n_seq // 4 - 1
    chunks = 3
    bits = [1 << b for b in reversed(range((n_tp - 1).bit_length()))]
    steps = sorted(range(1, planes), key=lambda k: (k % 2 == 0, min(k, planes - k), k))

    def from_plane(step):
        return [(2 * ((z + step) % planes) + y, 2 * z + y) for z in range(planes) for y in (0, 1)]

    half_swap = [(s, s ^ 1) for s in range(n_seq)]
    pair_swap = [(s, s ^ 2) for s in range(n_seq)]
    quad_up = [(s, s + 4) for s in range(n_seq - 4)]

    def over_tp(own):
        got = {0: own}
        for bit in bits:
            swap = [(t, t ^ bit) for t in range(n_tp)]
            got.update({i ^ bit: lax.ppermute(v, "tp", swap) for i, v in list(got.items())})
        return [got[i] for i in range(n_tp)]

    def body(
        tokens, query_weight, key_weight, value_weight, gate_weight, decay_rate, norm_gain, out_weight
    ):
        tok_rows, width = tokens.shape
        heads = decay_rate.shape[0]
        hp = heads // 2
        size = query_weight.shape[1] // heads
        tp = lax.axis_index("tp")
        rank = lax.axis_index("seq")
        half = rank % 2
        plane = rank // 2
        par = plane % 2
        where = jnp.stack([plane, half, par, tp]).astype(jnp.int32)
        tp_bits = [(tp >> b) & 1 for b in range((n_tp - 1).bit_length())]
        flags = jnp.stack([half, par, *tp_bits] + [par] * (6 - len(tp_bits))).astype(F32)
        flags = jnp.broadcast_to(flags[:, None], (8, 128))
        groups = [(h, "kvq") for h in range(hp - 1)] + [(hp - 1, "kv"), (hp - 1, "q")]
        rows = key_weight.shape[0]

        tile = tok_rows // n_tp
        sizes = (tile // chunks,) * chunks
        mine = turn(where, tokens, planes, rows, tile, sizes, 1, 61)
        pieces = [None] * (n_tp * chunks)
        for c in range(chunks):
            got = over_tp(lax.ppermute(mine[c], "seq", pair_swap))
            for i in range(n_tp):
                pieces[i * chunks + c] = got[i]
        (own_tokens,) = turn(where, tokens, planes, rows, 0, (tok_rows,), 0, 52)

        below = -(-heads * gate_rows(rows)[0] // 8) * 8
        packed = call(
            functools.partial(pack_kernel, groups=groups, size=size, hp=hp),
            [
                jax.ShapeDtypeStruct((rows + (0 if g else below), len(names) * size), BF)
                for g, (_, names) in enumerate(groups)
                for _ in (0, 1)
            ],
            (flags, key_weight, value_weight, query_weight, gate_weight.T),
            cost(1e6, key_weight.size * 12),
            61,
        )

        def gather(g):
            keep, give = packed[2 * g], packed[2 * g + 1]
            got = {0: keep}
            for k in steps:
                got[k] = lax.ppermute(give if k % 2 else keep, "seq", from_plane(k))
            blocks = []
            for k in range(planes):
                blocks += [got[k], lax.ppermute(got[k], "seq", half_swap)]
            return blocks

        gathered = [gather(g) for g in range(len(groups))]

        rate = jnp.broadcast_to(jnp.pad(decay_rate, (0, 8 - heads))[:, None], (8, 128))
        within = call(
            functools.partial(decay_kernel, hp=hp, rows=rows),
            jax.ShapeDtypeStruct((8, tok_rows), F32),
            (flags, own_tokens, rate, *gathered[0]),
            cost(64 * tok_rows * width, 2 * tok_rows * width),
        )
        within_far = lax.ppermute(within, "seq", pair_swap)
        gain = norm_gain.reshape(heads, size)

        own_proj, far_proj = [], []
        for blocks in gathered:
            far_proj.append(project(flags, half == 0, pieces, blocks, n_tp))
            own_proj.append(project(flags, half == 0, [own_tokens], blocks, n_tp))
        proj = list(zip(own_proj, far_proj))
        acc = []

        def out(normed, head, other, last):
            return call(
                functools.partial(
                    out_kernel,
                    n_tp=n_tp,
                    heads=heads,
                    hp=hp,
                    head=head,
                    flags=other,
                    size=size,
                    acc=len(acc),
                ),
                jax.ShapeDtypeStruct((tok_rows, out_weight.shape[1]), BF if last else F32),
                (flags, out_weight, *normed, *acc),
                cost(
                    2 * tok_rows * size * n_tp * len(other) * out_weight.shape[1],
                    2 * out_weight.size,
                ),
                20,
            )

        for head in range(hp):
            kv = proj[head]
            q = proj[-1] if head == hp - 1 else kv
            local = call(
                functools.partial(state_kernel, head=head, hp=hp, size=size),
                jax.ShapeDtypeStruct((2, size + 8, size), F32),
                (kv[0], kv[1], within, within_far),
                cost(4 * tok_rows * size * size, 16 * tok_rows * size),
            )
            far = lax.ppermute(local, "seq", half_swap)
            start = []
            for _ in range(hops):
                quad = call(
                    functools.partial(quad_kernel, size=size),
                    jax.ShapeDtypeStruct((size, size), F32),
                    (flags, local, far, *start),
                    cost(1e6, 40 * size * size),
                )
                start = [lax.ppermute(quad, "seq", quad_up)]

            def mix(which):
                kvq = [a for b in which for a in (kv[b], q[b])]
                windows = [(within, within_far)[b] for b in which]
                shape = jax.ShapeDtypeStruct((tok_rows, size), BF)
                return call(
                    functools.partial(
                        mix_kernel,
                        which=which,
                        head=head,
                        hp=hp,
                        size=size,
                        tile=256 if tok_rows % 256 == 0 else tok_rows,
                        starts=len(start),
                    ),
                    [shape] * len(which),
                    (flags, *kvq, *windows, local, far, gain, *start),
                    cost(
                        4 * tok_rows * tok_rows * size * len(which),
                        12 * tok_rows * size,
                        tok_rows * tok_rows,
                    ),
                )

            if head < hp - 1:
                normed, normed_far = mix((0, 1))
                back = lax.ppermute(normed_far, "seq", pair_swap)
                both = over_tp(normed) + over_tp(back)
                acc = [out(both, head, (0, 1), False)]
            else:
                (normed_far,) = mix((1,))
                back = lax.ppermute(normed_far, "seq", pair_swap)
                (normed,) = mix((0,))
                acc = [out(over_tp(normed), head, (0,), False)]
                return out(over_tp(back), head, (1,), True)

    return jax.shard_map(
        body,
        mesh=mesh,
        in_specs=(
            P("seq", None),
            P("seq", "tp"),
            P("seq", "tp"),
            P("seq", "tp"),
            P("seq", "tp"),
            P("tp"),
            P("tp"),
            P(None, "tp"),
        ),
        out_specs=P("seq", "tp"),
        check_vma=False,
    )
```
